32 devices in a mesh: grp: 2 (over x), slc: 16 (over z, y, core).
Axes of the slice: x: 2, y: 2, z: 4, core: 2. Of those that a mesh axis runs over, the one named last changes fastest.
Arguments:
- stem_tensor: bfloat16 [1024, 1024], P('slc'), may hold values from -6 to 6
- branches: bfloat16 [16, 6, 2, 1024, 1024], P('slc'), may hold values from -0.1875 to 0.1875
- chain_order: int32 [6], replicated, may hold values from 0 to 5, each once
- index_map: int32 [6], replicated, may hold values from 0 to 5, each once
- bitstrings: int32 [128, 16], P('grp'), parts along dimension 0, may hold values from 0 to 1023
- slice_labels: int32 [32], P(('grp', 'slc')), parts along dimension 0, may hold values from 0 to 63, as said below
Outputs:
- amplitudes: float32 [2048, 1024], P(('grp', 'slc')), parts along dimension 0
The draws below stay inside these ranges and needn't reach their ends.
There are 2 independent parts, one for each index of `grp`. The reference program is written for one: setup_inputs(seed, part) draws one part's arguments, and reference() takes and returns one part's arrays. A program takes and returns all parts, laid end to end along the dimension named above; an argument that names none is the same for every part. Nothing has to cross between parts.
Inputs may be any that keep to these rules, and one draw needn't show every extreme that they name: `slice_labels`: the 16 labels are distinct. `index_map`: each step names a different bit. `chain_order`: each branch tensor is contracted once.
All inputs are finite; a program needn't handle non-finite values.
Results may differ from the reference program's by a relative error of at most 0.025.
Values may be sent and summed in bfloat16 or wider, within the bound.
No kernel may reach another device: no remote copies, remote signals or barrier semaphores. Data moves between devices by JAX's collectives and lax.ppermute only.
A program may use at most 128 MiB of HBM per device.

```python
import jax
import jax.numpy as jnp
from jax import lax

D = 1024
Q = 1024
NT = 6
BATCH = 64
M = 16
SLICES = 16


def draw_slice_labels(key, part):
    return jax.random.permutation(key, 2 ** NT)[:SLICES].astype(jnp.int32)


def place_ends(array, key, low, largest):
    longest = array.shape.index(max(array.shape))
    spots = []
    for shift in (0, 1):
        where = [jax.random.randint(jax.random.fold_in(key, axis), (), 0, length) for axis, length in enumerate(array.shape)]
        where[longest] = (where[longest] + shift) % array.shape[longest]
        spots.append(tuple(where))
    return array.at[spots[0]].set(low).at[spots[1]].set(largest)


def shard_levels(key, extent, pieces, least, largest):
    def one(axis_at, blocks):
        steps = jax.random.uniform(jax.random.fold_in(jax.random.fold_in(key, 6), axis_at), (blocks,), jnp.float32, least / len(pieces), largest / len(pieces))
        return jnp.repeat(jnp.exp(steps), extent[axis_at] // blocks).reshape((-1,) + (1,) * (len(extent) - axis_at - 1))

    loudness = one(*pieces[0])
    for cut in pieces[1:]:
        loudness = loudness * one(*cut)
    return loudness


def gaussian(key, extent, width, limit, cuts=(), kind=jnp.bfloat16):
    loudness = shard_levels(key, extent, cuts, -0.22, 0.18) if cuts else 1.0
    entries = jax.random.normal(key, extent, jnp.float32) * width * loudness
    return jnp.minimum(jnp.maximum(entries, -limit), limit).astype(kind)


def setup_inputs(seed: int = 0, part: int = 0) -> dict:
    seeds = jax.random.split(jax.random.key(seed), 7)
    own_keys = jax.random.split(jax.random.fold_in(seeds[6], part), 7)
    return {
        "stem_tensor": gaussian(seeds[0], (Q, D), 1.0, 6.0, ((0, 16),)),
        "branches": gaussian(seeds[1], (SLICES, NT, 2, D, D), D ** -0.5, 0.1875, ((0, 16),)),
        "chain_order": jax.random.permutation(seeds[2], NT).astype(jnp.int32),
        "index_map": jax.random.permutation(seeds[3], NT).astype(jnp.int32),
        "bitstrings": place_ends(jax.random.randint(own_keys[4], (BATCH, M), 0, Q), jax.random.fold_in(own_keys[4], 1), 0, Q - 1).astype(jnp.int32),
        "slice_labels": draw_slice_labels(jax.random.fold_in(jax.random.fold_in(seeds[6], part), 71), part),
    }


def slice_partial(selected, slot_branches, chain_order, index_map, slice_label):
    current = selected
    product = None
    for step_index in range(NT):
        which_bit = jnp.right_shift(slice_label, index_map[step_index]) & 1
        tensor_pick = slot_branches[chain_order[step_index], which_bit]
        product = jnp.dot(current, tensor_pick, preferred_element_type=jnp.float32)
        if step_index < NT - 1:
            current = product.astype(jnp.bfloat16)
    return product


def reference(stem_tensor, branches, chain_order, index_map, bitstrings, slice_labels):
    selected = jnp.take(stem_tensor, bitstrings.reshape(-1), axis=0)

    def add_slice(slot_index, accumulated):
        return accumulated + slice_partial(selected, branches[slot_index], chain_order, index_map, slice_labels[slot_index])

    initial = jnp.zeros((selected.shape[0], selected.shape[1]), jnp.float32)
    accumulated = lax.fori_loop(0, SLICES, add_slice, initial)
    return accumulated * (SLICES ** -0.5)
```

```python
import functools

import jax
import jax.numpy as jnp
from jax import lax
from jax.experimental import pallas as pl
from jax.experimental.pallas import tpu as pltpu
from jax.sharding import PartitionSpec as P


def swap(array, mask, size):
    return lax.ppermute(array, "slc", [(i, i ^ mask) for i in range(size)])


def pick(flag, first, second):
    return jnp.where(flag == 0, first, second)


def chain_body(flip, order_ref, map_ref, label_ref, branches_ref, after_ref, away_ref, keep_ref, tail_ref, full_ref, sems):
    slots, steps = branches_ref.shape[:2]
    width = tail_ref.shape[-1]
    me = lax.axis_index("slc")
    column = pl.multiple_of(((jnp.right_shift(me, 1) & 1) ^ flip) * width, width)

    def load(slot, step):
        which = jnp.right_shift(label_ref[slot], map_ref[step]) & 1
        source = branches_ref.at[slot, order_ref[step], which]
        if step == steps - 1:
            return pltpu.make_async_copy(source.at[:, pl.ds(column, width)], tail_ref, sems.at[step])
        return pltpu.make_async_copy(source, full_ref.at[step], sems.at[step])

    total = None
    for slot in range(slots):
        copies = [load(slot, step) for step in range(steps)]
        for copy in reversed(copies):
            copy.start()
        copies[-1].wait()
        current = tail_ref[...]
        for step in reversed(range(steps - 1)):
            copies[step].wait()
            product = jnp.dot(full_ref[step], current, preferred_element_type=jnp.float32)
            current = product.astype(jnp.bfloat16)
        total = product if total is None else total + product
    total = total.astype(jnp.bfloat16)
    left, right = total[:, : width // 2], total[:, width // 2 :]
    first = (me & 1) == 0
    away_ref[...] = jnp.where(first, right, left)
    keep_ref[...] = jnp.where(first, left, right)


def chain_columns(flip, scalars, branches, after):
    steps, bond = branches.shape[1], branches.shape[-1]
    smem = pl.BlockSpec(memory_space=pltpu.SMEM)
    vmem = pl.BlockSpec(memory_space=pltpu.VMEM)
    quarter = jax.ShapeDtypeStruct((bond, bond // 4), jnp.bfloat16)
    return pl.pallas_call(
        functools.partial(chain_body, flip),
        out_shape=(quarter, quarter),
        in_specs=[smem, smem, smem, pl.BlockSpec(memory_space=pl.ANY), pl.BlockSpec(memory_space=pl.ANY)],
        out_specs=(vmem, vmem),
        scratch_shapes=[
            pltpu.VMEM((bond, bond // 2), jnp.bfloat16),
            pltpu.VMEM((steps - 1, bond, bond), jnp.bfloat16),
            pltpu.SemaphoreType.DMA((steps,)),
        ],
        cost_estimate=pl.CostEstimate(
            flops=branches.size * bond // 2, bytes_accessed=branches.size, transcendentals=0
        ),
    )(*scalars, branches, after)


def amplitudes(stem_tensor, branches, chain_order, index_map, bitstrings, slice_labels):
    size = lax.axis_size("slc")
    me = lax.axis_index("slc")
    scalars = (chain_order, index_map, slice_labels)

    pair = jnp.concatenate([stem_tensor, swap(stem_tensor, 2, size)], axis=0)
    near_rows = jnp.concatenate([pair] + [swap(pair, mask, size) for mask in range(4, size, 4)], axis=0)
    gathered = jnp.concatenate([near_rows, swap(near_rows, 1, size)], axis=0)

    away, keep = chain_columns(1, scalars, branches, pair)
    far = (keep.astype(jnp.float32) + swap(away, 1, size).astype(jnp.float32)).astype(jnp.bfloat16)
    away, keep = chain_columns(0, scalars, branches, far)
    far = swap(far, 2, size)
    own = keep.astype(jnp.float32) + swap(away, 1, size).astype(jnp.float32)
    own = (own + far.astype(jnp.float32)).astype(jnp.bfloat16)

    flat = bitstrings.reshape(-1)
    rows = stem_tensor.shape[0]
    owner = (flat // rows) ^ me
    place = (jnp.right_shift(owner, 1) + (owner & 1) * (size // 2)) * rows + flat % rows
    hot = (place[:, None] == lax.broadcasted_iota(jnp.int32, (flat.shape[0], rows * size), 1)).astype(jnp.bfloat16)

    every = jnp.dot(gathered, own, preferred_element_type=jnp.float32).astype(jnp.bfloat16)
    part = jnp.dot(hot, every, preferred_element_type=jnp.float32).astype(jnp.bfloat16)

    groups = size // 4
    mine = jnp.right_shift(me, 2)
    blocks = part.reshape(groups, part.shape[0] // groups, part.shape[1])
    total = lax.dynamic_index_in_dim(blocks, mine, 0, keepdims=False).astype(jnp.float32)
    for mask in range(1, groups):
        sent = lax.dynamic_index_in_dim(blocks, mine ^ mask, 0, keepdims=False)
        total = total + swap(sent, 4 * mask, size).astype(jnp.float32)

    normalizer = float(slice_labels.shape[0] * size) ** (-0.5)
    quarter = me & 3
    kept = total.astype(jnp.bfloat16).reshape(4, total.shape[0] // 4, total.shape[1])
    got = []
    for mask in range(4):
        sent = lax.dynamic_index_in_dim(kept, quarter ^ mask, 0, keepdims=False)
        got.append(swap(sent, mask, size) if mask else sent)
    low, high = quarter & 1, jnp.right_shift(quarter, 1)
    pairs = [(pick(low, got[m], got[m + 1]), pick(low, got[m + 1], got[m])) for m in (0, 2)]
    columns = [pick(high, pairs[0][i], pairs[1][i]) for i in (0, 1)] + [pick(high, pairs[1][i], pairs[0][i]) for i in (0, 1)]
    return jnp.concatenate(columns, axis=1).astype(jnp.float32) * normalizer


def solution(mesh):
    placed = (
        P("slc", None),
        P("slc", None, None, None, None),
        P(),
        P(),
        P("grp", None),
        P(("grp", "slc")),
    )
    return jax.shard_map(amplitudes, mesh=mesh, in_specs=placed, out_specs=P(("grp", "slc"), None), check_vma=False)
```
